32 devices in a mesh: rows: 32 (over z, y, x, core).
Axes of the slice: x: 2, y: 2, z: 4, core: 2. Of those that a mesh axis runs over, the one named last changes fastest.
Arguments:
- points: float32 [8, 131072], P(None, 'rows'), may hold values from -6 to 6
- scales: float32 [8], replicated, may hold values from 1 to 3
- noise_var: float32 [131072], P('rows'), may hold values from 0.05 to 0.5
- pivots: int32 [8, 16], replicated, may hold values from 0 to 131071, as said below
Outputs:
- factor: float32 [128, 131072], P(None, 'rows')
- residual_diag: float32 [131072], P('rows')
- mean_residual: float32 [8], replicated
The draws below stay inside these ranges and needn't reach their ends.
Inputs may be any that keep to these rules, and one draw needn't show every extreme that they name: `pivots`: all 128 entries are distinct point indices.
All inputs are finite; a program needn't handle non-finite values.
Results may differ from the reference program's by a relative error of at most 0.00014.
Values sent between devices are 32-bit elements; how exact they have to be, the bound alone decides.
A program may use at most 64 MiB of HBM per device.

```python
import math
import jax
import jax.numpy as jnp
from jax import lax

DIM = 8
BS = 16
BLOCKS = 8
NPTS = 131072


def draw_pivots(key, part):
    chosen = jax.random.permutation(key, NPTS)[:BLOCKS * BS]
    return chosen.reshape((BLOCKS, BS)).astype(jnp.int32)


def block_scale(own_key, extent, split, low, top_value):
    level = 1.0
    for dim, parts in split:
        draws = jax.random.uniform(jax.random.fold_in(jax.random.fold_in(own_key, 6), dim), (parts,), jnp.float32, low / len(split), top_value / len(split))
        level = level * jnp.repeat(jnp.exp(draws), extent[dim] // parts).reshape((-1,) + (1,) * (len(extent) - 1 - dim))
    return level


def centred(own_key, dims, width, reach, split=(), kind=jnp.bfloat16):
    array = jax.random.normal(own_key, dims, jnp.float32) * width
    if len(split) > 0:
        array = block_scale(own_key, dims, split, -0.22, 0.18) * array
    return jnp.clip(array, min=-reach, max=reach).astype(kind)


def setup_inputs(seed: int = 0) -> dict:
    keys = jax.random.split(jax.random.key(seed), 5)
    points = centred(keys[0], (DIM, NPTS), 1.0, 6.0, ((1, 32),), jnp.float32)
    scales = jnp.clip(jnp.exp(jax.random.uniform(keys[1], (DIM,), jnp.float32, math.log(1.0), math.log(3.0))), 1.0, 3.0)
    noise_var = jnp.clip(jnp.exp(math.log(0.5) - 2.3025851 * jax.random.uniform(keys[2], (NPTS,), jnp.float32) ** block_scale(keys[2], (NPTS,), ((0, 32),), -0.2, 0.2)), 0.05, 0.5)
    pivots = draw_pivots(jax.random.fold_in(keys[4], 71), 0)
    return dict(points=points, scales=scales, noise_var=noise_var, pivots=pivots)


def kernel(first_coords, second_coords):
    summed = jnp.zeros((first_coords.shape[1], second_coords.shape[1]), jnp.float32)
    for axis_pos in range(first_coords.shape[0]):
        differ = first_coords[axis_pos][:, None] - second_coords[axis_pos][None, :]
        summed = summed + differ * differ
    return jnp.exp(-0.5 * summed)

def reference(points, scales, noise_var, pivots):
    scaled = points / scales[:, None]
    point_count = points.shape[1]
    point_ids = jnp.arange(point_count, dtype=jnp.int32)
    residual_diag = 1.0 + noise_var
    done_rows = []
    averages = []
    for block_idx in range(BLOCKS):
        wanted = pivots[block_idx]
        pivot_coords = jnp.take(scaled, wanted, axis=1)
        columns = kernel(pivot_coords, scaled) + jnp.where(point_ids[None, :] == wanted[:, None], noise_var[None, :], 0.0)
        for earlier in done_rows:
            picked = jnp.take(earlier, wanted, axis=1)
            columns = columns - jnp.dot(picked.T.astype(jnp.float32), earlier.astype(jnp.float32), precision=lax.Precision.HIGHEST, preferred_element_type=jnp.float32)
        pivot_block = jnp.take(columns, wanted, axis=1)
        chol_block = jnp.linalg.cholesky(pivot_block)
        new_rows = lax.linalg.triangular_solve(chol_block, columns, left_side=True, lower=True)
        done_rows.append(new_rows)
        residual_diag = residual_diag - jnp.sum(new_rows * new_rows, axis=0)
        averages.append(jnp.sum(residual_diag) / point_count)
    return (jnp.concatenate(done_rows, axis=0), residual_diag, jnp.stack(averages))
```

```python
import functools

import jax
import jax.numpy as jnp
from jax import lax
from jax.experimental import pallas as pl
from jax.experimental.pallas import tpu as pltpu
from jax.sharding import PartitionSpec as P

LANES = 128
SUB = 8
F32 = jnp.float32
BF16 = jnp.bfloat16


def split3(x):
    high = x.astype(BF16).astype(F32)
    rest = x - high
    mid = rest.astype(BF16).astype(F32)
    low = (rest - mid).astype(BF16).astype(F32)
    return high, mid, low


def load_points(dim, points, scales, noise, packed):
    packed[0:dim, :] = points[...] / scales[...]
    packed[dim : 2 * dim, :] = jnp.broadcast_to(noise[...], (dim, noise.shape[1]))


def gather_own(ranks, offset, chunk, pivot_row, packed):
    rows, width = packed.shape
    wanted = pivot_row[...] - offset
    acc = jnp.zeros((3 * rows, ranks), F32)
    for c in range(width // chunk):
        pieces = jnp.concatenate(split3(packed[:, c * chunk : (c + 1) * chunk]), axis=0)
        ids = lax.broadcasted_iota(jnp.int32, (chunk, ranks), 0) + c * chunk
        hot = jnp.where(ids == wanted, 1.0, 0.0).astype(BF16)
        acc = acc + jnp.dot(pieces.astype(BF16), hot, preferred_element_type=F32)
    return acc[0:rows] + acc[rows : 2 * rows] + acc[2 * rows :]


def exchange_start(n, me, slots, send_sem, recv_sem):
    def send(k, carry):
        pltpu.make_async_remote_copy(
            src_ref=slots.at[0],
            dst_ref=slots.at[k],
            send_sem=send_sem.at[k],
            recv_sem=recv_sem.at[k],
            device_id=(lax.rem(me + k, n),),
            device_id_type=pl.DeviceIdType.MESH,
        ).start()
        return carry

    lax.fori_loop(1, n, send, 0)


def exchange_finish(n, me, slots, send_sem, recv_sem):
    def collect(k, total):
        pltpu.make_async_remote_copy(
            src_ref=slots.at[0],
            dst_ref=slots.at[k],
            send_sem=send_sem.at[k],
            recv_sem=recv_sem.at[k],
            device_id=(lax.rem(me + k, n),),
            device_id_type=pl.DeviceIdType.MESH,
        ).wait()
        return total + slots[k]

    return lax.fori_loop(1, n, collect, slots[0])


def pivot_covariance(dim, coords):
    ranks = coords.shape[1]
    across = coords.T
    total = jnp.zeros((ranks, ranks), F32)
    for d in range(dim):
        differ = across[:, d : d + 1] - coords[d : d + 1, :]
        total = total + differ * differ
    row = lax.broadcasted_iota(jnp.int32, (ranks, ranks), 0)
    col = lax.broadcasted_iota(jnp.int32, (ranks, ranks), 1)
    cov = jnp.exp(-0.5 * total) + jnp.where(row == col, coords[dim : dim + 1, :], 0.0)
    return cov, (row == col).astype(F32)


def factor_rows(ranks, state):
    for b in range(ranks // SUB):
        lo, hi = b * SUB, (b + 1) * SUB
        left = [state[lo + i : lo + i + 1, 0:ranks] for i in range(SUB)]
        right = [state[lo + i : lo + i + 1, ranks : 2 * ranks] for i in range(SUB)]
        a = [
            [jnp.broadcast_to(left[i][:, lo + j : lo + j + 1], (1, ranks)) for j in range(i + 1)]
            for i in range(SUB)
        ]
        for k in range(SUB):
            r = lax.rsqrt(a[k][k])
            left[k] = left[k] * r
            right[k] = right[k] * r
            mult = {i: a[i][k] * r for i in range(k + 1, SUB)}
            for i in range(k + 1, SUB):
                for j in range(k + 1, i + 1):
                    a[i][j] = a[i][j] - mult[i] * mult[j]
                left[i] = left[i] - mult[i] * left[k]
                right[i] = right[i] - mult[i] * right[k]
        new_left = jnp.concatenate(left, axis=0)
        new_right = jnp.concatenate(right, axis=0)
        state[lo:hi, 0:ranks] = new_left
        state[lo:hi, ranks : 2 * ranks] = new_right
        if hi < ranks:
            new = jnp.concatenate([new_left, new_right], axis=1)
            h, m, l = split3(new)
            lh, lm, ll = (x[:, 0:ranks] for x in (h, m, l))
            one = jnp.concatenate([lh, lh, lh, lm, lm, ll], axis=0).T[hi:ranks].astype(BF16)
            two = jnp.concatenate([h, m, l, h, m, h], axis=0).astype(BF16)
            state[hi:ranks, :] = state[hi:ranks, :] - jnp.dot(
                one, two, preferred_element_type=F32
            )


def pivot_side(dim, coords, centre):
    y = coords[0:dim, :] - centre
    yh, ym, yl = split3(y)
    nh, nm, nl = split3(-0.5 * jnp.sum(y * y, axis=0, keepdims=True))
    ones = jnp.ones_like(nh)
    tail = [ones, ones, ones, nh, nm, nl, jnp.zeros((dim - 6, y.shape[1]), F32)]
    return jnp.concatenate([yh, yh, ym, ym, yh, yl] + tail, axis=0).T.astype(BF16)


def point_side(dim, x):
    xh, xm, xl = split3(x)
    nh, nm, nl = split3(-0.5 * jnp.sum(x * x, axis=0, keepdims=True))
    ones = jnp.ones_like(nh)
    tail = [nh, nm, nl, ones, ones, ones, jnp.zeros((dim - 6, x.shape[1]), F32)]
    return jnp.concatenate([xh, xm, xh, xm, xl, xh] + tail, axis=0).astype(BF16)


def body_kernel(
    n, blocks, chunk,
    points, scales, noise, pivot_row, pivot_col,
    factor, residual, averages,
    packed, slots, state, held, after, sum_slots,
    send_sem, recv_sem, sum_send_sem, sum_recv_sem, out_sem,
):
    dim, width = points.shape
    ranks = held.shape[0]
    per_block = ranks // blocks
    me = lax.axis_index("rows")
    offset = me * width

    barrier = pltpu.get_barrier_semaphore()

    def greet(k, carry):
        pl.semaphore_signal(
            barrier, inc=1, device_id=(lax.rem(me + k, n),),
            device_id_type=pl.DeviceIdType.MESH,
        )
        return carry

    lax.fori_loop(1, n, greet, 0)
    load_points(dim, points, scales, noise, packed)
    slots[0] = gather_own(ranks, offset, chunk, pivot_row, packed)
    pl.semaphore_wait(barrier, n - 1)
    exchange_start(n, me, slots, send_sem, recv_sem)
    coords = exchange_finish(n, me, slots, send_sem, recv_sem)

    cov, eye = pivot_covariance(dim, coords)
    state[:, 0:ranks] = cov
    state[:, ranks : 2 * ranks] = eye
    factor_rows(ranks, state)
    row = lax.broadcasted_iota(jnp.int32, (ranks, ranks), 0)
    col = lax.broadcasted_iota(jnp.int32, (ranks, ranks), 1)
    solve = jnp.where(row >= col, state[:, ranks : 2 * ranks], 0.0)

    centre = jnp.sum(coords[0:dim, :], axis=1, keepdims=True) / ranks
    side = pivot_side(dim, coords, centre)
    local_col = pivot_col[...] - offset
    copies = []
    for c in range(width // chunk):
        at = slice(c * chunk, (c + 1) * chunk)
        x = packed[0:dim, at] - centre
        cross = jnp.exp(jnp.dot(side, point_side(dim, x), preferred_element_type=F32))
        noise_row = packed[dim : dim + 1, at]
        ids = lax.broadcasted_iota(jnp.int32, (ranks, chunk), 1) + c * chunk
        cross = cross + jnp.where(ids == local_col, noise_row, 0.0)
        rows = jnp.dot(
            solve, cross, precision=lax.Precision.HIGHEST, preferred_element_type=F32
        )
        held[:, at] = rows
        copies.append(
            pltpu.make_async_copy(held.at[:, at], factor.at[:, at], out_sem.at[c])
        )
        copies[-1].start()
        left = 1.0 + noise_row
        for b in range(blocks):
            part = rows[b * per_block : (b + 1) * per_block]
            left = left - jnp.sum(part * part, axis=0, keepdims=True)
            after[b : b + 1, at] = left
        residual[:, at] = left

    total = jnp.zeros((blocks, LANES), F32)
    for c in range(width // LANES):
        total = total + after[:, c * LANES : (c + 1) * LANES]
    sum_slots[0] = total
    exchange_start(n, me, sum_slots, sum_send_sem, sum_recv_sem)
    total = exchange_finish(n, me, sum_slots, sum_send_sem, sum_recv_sem)
    total = jnp.sum(total, axis=1, keepdims=True) / (width * n)
    row = lax.broadcasted_iota(jnp.int32, (blocks, LANES), 0)
    col = lax.broadcasted_iota(jnp.int32, (blocks, LANES), 1)
    averages[...] = jnp.sum(jnp.where(row == col, total, 0.0), axis=0, keepdims=True)[:, 0:blocks]
    for copy in copies:
        copy.wait()


def body(n, points, scales, noise_var, pivots):
    dim, width = points.shape
    blocks, per_block = pivots.shape
    ranks = blocks * per_block
    chunk = 512
    vmem = pl.BlockSpec(memory_space=pltpu.VMEM)
    flat = pivots.reshape(-1)
    factor, residual, averages = pl.pallas_call(
        functools.partial(body_kernel, n, blocks, chunk),
        name="whole",
        out_shape=(
            jax.ShapeDtypeStruct((ranks, width), F32),
            jax.ShapeDtypeStruct((1, width), F32),
            jax.ShapeDtypeStruct((1, blocks), F32),
        ),
        in_specs=[vmem] * 5,
        out_specs=(pl.BlockSpec(memory_space=pl.ANY), vmem, vmem),
        scratch_shapes=[
            pltpu.VMEM((2 * dim, width), F32),
            pltpu.VMEM((n, 2 * dim, ranks), F32),
            pltpu.VMEM((ranks, 2 * ranks), F32),
            pltpu.VMEM((ranks, width), F32),
            pltpu.VMEM((blocks, width), F32),
            pltpu.VMEM((n, blocks, LANES), F32),
            pltpu.SemaphoreType.DMA((n,)),
            pltpu.SemaphoreType.DMA((n,)),
            pltpu.SemaphoreType.DMA((n,)),
            pltpu.SemaphoreType.DMA((n,)),
            pltpu.SemaphoreType.DMA((width // chunk,)),
        ],
        compiler_params=pltpu.CompilerParams(collective_id=0, has_side_effects=True),
    )(
        points, scales.reshape(-1, 1), noise_var.reshape(1, -1),
        flat.reshape(1, -1), flat.reshape(-1, 1),
    )
    return factor, residual.reshape(-1), averages.reshape(-1)


def solution(mesh):
    in_specs = (P(None, "rows"), P(), P("rows"), P())
    out_specs = (P(None, "rows"), P("rows"), P())
    return jax.shard_map(
        functools.partial(body, mesh.shape["rows"]),
        mesh=mesh, in_specs=in_specs, out_specs=out_specs, check_vma=False,
    )
```

```python
import functools

import jax
import jax.numpy as jnp
from jax import lax
from jax.experimental import pallas as pl
from jax.experimental.pallas import tpu as pltpu
from jax.sharding import PartitionSpec as P

LANES = 128
SUB = 8
F32 = jnp.float32
BF16 = jnp.bfloat16


def split3(x):
    high = x.astype(BF16).astype(F32)
    rest = x - high
    mid = rest.astype(BF16).astype(F32)
    low = (rest - mid).astype(BF16).astype(F32)
    return high, mid, low


def load_points(dim, points, scales, noise, packed):
    axis_pos = lax.broadcasted_iota(jnp.int32, (dim, 1), 0)
    scale = jnp.ones((dim, 1), F32)
    for d in range(dim):
        scale = jnp.where(axis_pos == d, scales[d], scale)
    packed[0:dim, :] = points[...] / scale
    packed[dim : 2 * dim, :] = jnp.broadcast_to(noise[...], (dim, noise.shape[1]))


def gather_own(ranks, offset, chunk, pivot_row, packed):
    rows, width = packed.shape
    wanted = pivot_row - offset
    acc = jnp.zeros((3 * rows, ranks), F32)
    for c in range(width // chunk):
        pieces = jnp.concatenate(split3(packed[:, c * chunk : (c + 1) * chunk]), axis=0)
        ids = lax.broadcasted_iota(jnp.int32, (chunk, ranks), 0) + c * chunk
        hot = jnp.where(ids == wanted, 1.0, 0.0).astype(BF16)
        acc = acc + jnp.dot(pieces.astype(BF16), hot, preferred_element_type=F32)
    return acc[0:rows] + acc[rows : 2 * rows] + acc[2 * rows :]


def exchange_start(n, me, slots, send_sem, recv_sem):
    def send(k, carry):
        pltpu.make_async_remote_copy(
            src_ref=slots.at[0],
            dst_ref=slots.at[k],
            send_sem=send_sem.at[k],
            recv_sem=recv_sem.at[k],
            device_id=(lax.rem(me + k, n),),
            device_id_type=pl.DeviceIdType.MESH,
        ).start()
        return carry

    lax.fori_loop(1, n, send, 0)


def exchange_finish(n, me, slots, send_sem, recv_sem):
    def collect(k, total):
        pltpu.make_async_remote_copy(
            src_ref=slots.at[0],
            dst_ref=slots.at[k],
            send_sem=send_sem.at[k],
            recv_sem=recv_sem.at[k],
            device_id=(lax.rem(me + k, n),),
            device_id_type=pl.DeviceIdType.MESH,
        ).wait()
        return total + slots[k]

    return lax.fori_loop(1, n, collect, slots[0])


def pivot_covariance(dim, coords):
    ranks = coords.shape[1]
    across = coords.T
    total = jnp.zeros((ranks, ranks), F32)
    for d in range(dim):
        differ = across[:, d : d + 1] - coords[d : d + 1, :]
        total = total + differ * differ
    row = lax.broadcasted_iota(jnp.int32, (ranks, ranks), 0)
    col = lax.broadcasted_iota(jnp.int32, (ranks, ranks), 1)
    cov = jnp.exp(-0.5 * total) + jnp.where(row == col, coords[dim : dim + 1, :], 0.0)
    return cov, (row == col).astype(F32)


def factor_rows(ranks, state):
    for b in range(ranks // SUB):
        lo, hi = b * SUB, (b + 1) * SUB
        left = [state[lo + i : lo + i + 1, 0:ranks] for i in range(SUB)]
        right = [state[lo + i : lo + i + 1, ranks : 2 * ranks] for i in range(SUB)]
        a = [
            [jnp.broadcast_to(left[i][:, lo + j : lo + j + 1], (1, ranks)) for j in range(i + 1)]
            for i in range(SUB)
        ]
        for k in range(SUB):
            r = lax.rsqrt(a[k][k])
            left[k] = left[k] * r
            right[k] = right[k] * r
            mult = {i: a[i][k] * r for i in range(k + 1, SUB)}
            for i in range(k + 1, SUB):
                for j in range(k + 1, i + 1):
                    a[i][j] = a[i][j] - mult[i] * mult[j]
                left[i] = left[i] - mult[i] * left[k]
                right[i] = right[i] - mult[i] * right[k]
        new_left = jnp.concatenate(left, axis=0)
        new_right = jnp.concatenate(right, axis=0)
        state[lo:hi, 0:ranks] = new_left
        state[lo:hi, ranks : 2 * ranks] = new_right
        if hi < ranks:
            new = jnp.concatenate([new_left, new_right], axis=1)
            h, m, l = split3(new)
            lh, lm, ll = (x[:, 0:ranks] for x in (h, m, l))
            one = jnp.concatenate([lh, lh, lh, lm, lm, ll], axis=0).T[hi:ranks].astype(BF16)
            two = jnp.concatenate([h, m, l, h, m, h], axis=0).astype(BF16)
            state[hi:ranks, :] = state[hi:ranks, :] - jnp.dot(
                one, two, preferred_element_type=F32
            )


def pivot_side(dim, coords, centre):
    y = coords[0:dim, :] - centre
    yh, ym, yl = split3(y)
    nh, nm, nl = split3(-0.5 * jnp.sum(y * y, axis=0, keepdims=True))
    ones = jnp.ones_like(nh)
    tail = [ones, ones, ones, nh, nm, nl, jnp.zeros((dim - 6, y.shape[1]), F32)]
    return jnp.concatenate([yh, yh, ym, ym, yh, yl] + tail, axis=0).T.astype(BF16)


def point_side(dim, x):
    xh, xm, xl = split3(x)
    nh, nm, nl = split3(-0.5 * jnp.sum(x * x, axis=0, keepdims=True))
    ones = jnp.ones_like(nh)
    tail = [nh, nm, nl, ones, ones, ones, jnp.zeros((dim - 6, x.shape[1]), F32)]
    return jnp.concatenate([xh, xm, xh, xm, xl, xh] + tail, axis=0).astype(BF16)


def body_kernel(
    n, blocks, chunk,
    points, scales, noise, pivots, unset_factor,
    factor, residual, averages,
    packed, slots, state, held, after, sum_slots,
    send_sem, recv_sem, sum_send_sem, sum_recv_sem, out_sem,
):
    dim, width = points.shape
    ranks = held.shape[0]
    per_block = ranks // blocks
    me = lax.axis_index("rows")
    offset = me * width

    barrier = pltpu.get_barrier_semaphore()

    def greet(k, carry):
        pl.semaphore_signal(
            barrier, inc=1, device_id=(lax.rem(me + k, n),),
            device_id_type=pl.DeviceIdType.MESH,
        )
        return carry

    lax.fori_loop(1, n, greet, 0)
    load_points(dim, points, scales, noise, packed)
    pivot_row = jnp.concatenate([pivots[b : b + 1, :] for b in range(blocks)], axis=1)
    own = gather_own(ranks, offset, chunk, pivot_row, packed)
    for d in range(dim + 1):
        slots[0, d] = own[d : d + 1]
    pl.semaphore_wait(barrier, n - 1)
    exchange_start(n, me, slots, send_sem, recv_sem)
    coords = exchange_finish(n, me, slots, send_sem, recv_sem)
    coords = jnp.concatenate([coords[d] for d in range(dim + 1)], axis=0)

    cov, eye = pivot_covariance(dim, coords)
    state[:, 0:ranks] = cov
    state[:, ranks : 2 * ranks] = eye
    factor_rows(ranks, state)
    row = lax.broadcasted_iota(jnp.int32, (ranks, ranks), 0)
    col = lax.broadcasted_iota(jnp.int32, (ranks, ranks), 1)
    solve = jnp.where(row >= col, state[:, ranks : 2 * ranks], 0.0)

    centre = jnp.sum(coords[0:dim, :], axis=1, keepdims=True) / ranks
    side = pivot_side(dim, coords, centre)
    local_row = (pivot_row - offset).astype(F32)
    local_col = jnp.broadcast_to(local_row, (SUB, ranks)).T[:, 0:1].astype(jnp.int32)
    copies = []
    for c in range(width // chunk):
        at = slice(c * chunk, (c + 1) * chunk)
        x = packed[0:dim, at] - centre
        cross = jnp.exp(jnp.dot(side, point_side(dim, x), preferred_element_type=F32))
        noise_row = packed[dim : dim + 1, at]
        ids = lax.broadcasted_iota(jnp.int32, (ranks, chunk), 1) + c * chunk
        cross = cross + jnp.where(ids == local_col, noise_row, 0.0)
        rows = jnp.dot(
            solve, cross, precision=lax.Precision.HIGHEST, preferred_element_type=F32
        )
        held[:, at] = rows
        copies.append(
            pltpu.make_async_copy(held.at[:, at], factor.at[:, at], out_sem.at[c])
        )
        copies[-1].start()
        left = 1.0 + noise_row
        for b in range(blocks):
            part = rows[b * per_block : (b + 1) * per_block]
            left = left - jnp.sum(part * part, axis=0, keepdims=True)
            after[b : b + 1, at] = left
        residual[:, at] = left

    total = jnp.zeros((blocks, LANES), F32)
    for c in range(width // LANES):
        total = total + after[:, c * LANES : (c + 1) * LANES]
    total = jnp.sum(total, axis=1, keepdims=True)
    row = lax.broadcasted_iota(jnp.int32, (blocks, LANES), 0)
    col = lax.broadcasted_iota(jnp.int32, (blocks, LANES), 1)
    sum_slots[0] = jnp.sum(jnp.where(row == col, total, 0.0), axis=0, keepdims=True)
    exchange_start(n, me, sum_slots, sum_send_sem, sum_recv_sem)
    total = exchange_finish(n, me, sum_slots, sum_send_sem, sum_recv_sem)
    averages[...] = total[:, 0:blocks] / (width * n)
    for copy in copies:
        copy.wait()


def body(n, points, scales, noise_var, pivots):
    dim, width = points.shape
    blocks, per_block = pivots.shape
    ranks = blocks * per_block
    chunk = 512
    vmem = pl.BlockSpec(memory_space=pltpu.VMEM)
    unset = pl.pallas_call(
        lambda out: None,
        name="unset",
        out_shape=jax.ShapeDtypeStruct((ranks, width), F32),
        out_specs=pl.BlockSpec(memory_space=pl.ANY),
    )()
    factor, residual, averages = pl.pallas_call(
        functools.partial(body_kernel, n, blocks, chunk),
        name="whole",
        out_shape=(
            jax.ShapeDtypeStruct((ranks, width), F32),
            jax.ShapeDtypeStruct((1, width), F32),
            jax.ShapeDtypeStruct((1, blocks), F32),
        ),
        in_specs=[
            vmem, pl.BlockSpec(memory_space=pltpu.SMEM), vmem, vmem,
            pl.BlockSpec(memory_space=pl.ANY),
        ],
        input_output_aliases={4: 0},
        out_specs=(pl.BlockSpec(memory_space=pl.ANY), vmem, vmem),
        scratch_shapes=[
            pltpu.VMEM((2 * dim, width), F32),
            pltpu.VMEM((n, dim + 1, 1, ranks), F32),
            pltpu.VMEM((ranks, 2 * ranks), F32),
            pltpu.VMEM((ranks, width), F32),
            pltpu.VMEM((blocks, width), F32),
            pltpu.VMEM((n, 1, LANES), F32),
            pltpu.SemaphoreType.DMA((n,)),
            pltpu.SemaphoreType.DMA((n,)),
            pltpu.SemaphoreType.DMA((n,)),
            pltpu.SemaphoreType.DMA((n,)),
            pltpu.SemaphoreType.DMA((width // chunk,)),
        ],
        compiler_params=pltpu.CompilerParams(collective_id=0, has_side_effects=True),
    )(points, scales, noise_var.reshape(1, -1), pivots, unset)
    return factor, residual.reshape(-1), averages.reshape(-1)


def solution(mesh):
    in_specs = (P(None, "rows"), P(), P("rows"), P())
    out_specs = (P(None, "rows"), P("rows"), P())
    return jax.shard_map(
        functools.partial(body, mesh.shape["rows"]),
        mesh=mesh, in_specs=in_specs, out_specs=out_specs, check_vma=False,
    )
```

```python
import functools

import jax
import jax.numpy as jnp
from jax import lax
from jax.experimental import pallas as pl
from jax.experimental.pallas import tpu as pltpu
from jax.sharding import PartitionSpec as P

LANES = 128
SUB = 8
F32 = jnp.float32
BF16 = jnp.bfloat16


def split3(x):
    high = x.astype(BF16).astype(F32)
    rest = x - high
    mid = rest.astype(BF16).astype(F32)
    low = (rest - mid).astype(BF16).astype(F32)
    return high, mid, low


def load_points(dim, points, scales, noise, packed):
    axis_pos = lax.broadcasted_iota(jnp.int32, (dim, 1), 0)
    scale = jnp.ones((dim, 1), F32)
    for d in range(dim):
        scale = jnp.where(axis_pos == d, scales[d], scale)
    packed[0:dim, :] = points[...] / scale
    packed[dim : 2 * dim, :] = jnp.broadcast_to(noise[...], (dim, noise.shape[1]))


def gather_own(ranks, offset, chunk, pivot_row, packed):
    rows, width = packed.shape
    wanted = pivot_row - offset
    acc = jnp.zeros((3 * rows, ranks), F32)
    for c in range(width // chunk):
        pieces = jnp.concatenate(split3(packed[:, c * chunk : (c + 1) * chunk]), axis=0)
        ids = lax.broadcasted_iota(jnp.int32, (chunk, ranks), 0) + c * chunk
        hot = jnp.where(ids == wanted, 1.0, 0.0).astype(BF16)
        acc = acc + jnp.dot(pieces.astype(BF16), hot, preferred_element_type=F32)
    return acc[0:rows] + acc[rows : 2 * rows] + acc[2 * rows :]


def exchange_start(n, me, slots, send_sem, recv_sem):
    def send(k, carry):
        pltpu.make_async_remote_copy(
            src_ref=slots.at[0],
            dst_ref=slots.at[k],
            send_sem=send_sem.at[k],
            recv_sem=recv_sem.at[k],
            device_id=(lax.rem(me + k, n),),
            device_id_type=pl.DeviceIdType.MESH,
        ).start()
        return carry

    lax.fori_loop(1, n, send, 0)


def exchange_finish(n, me, slots, send_sem, recv_sem):
    def collect(k, total):
        pltpu.make_async_remote_copy(
            src_ref=slots.at[0],
            dst_ref=slots.at[k],
            send_sem=send_sem.at[k],
            recv_sem=recv_sem.at[k],
            device_id=(lax.rem(me + k, n),),
            device_id_type=pl.DeviceIdType.MESH,
        ).wait()
        return total + slots[k]

    return lax.fori_loop(1, n, collect, slots[0])


def pivot_covariance(dim, coords):
    ranks = coords.shape[1]
    across = coords.T
    total = jnp.zeros((ranks, ranks), F32)
    for d in range(dim):
        differ = across[:, d : d + 1] - coords[d : d + 1, :]
        total = total + differ * differ
    row = lax.broadcasted_iota(jnp.int32, (ranks, ranks), 0)
    col = lax.broadcasted_iota(jnp.int32, (ranks, ranks), 1)
    cov = jnp.exp(-0.5 * total) + jnp.where(row == col, coords[dim : dim + 1, :], 0.0)
    return cov, (row == col).astype(F32)


def eliminate(left, right, first_lane):
    shape = left[0].shape
    a = [
        [
            jnp.broadcast_to(left[i][:, first_lane + j : first_lane + j + 1], shape)
            for j in range(i + 1)
        ]
        for i in range(SUB)
    ]
    inverse = []
    for k in range(SUB):
        r = lax.rsqrt(a[k][k])
        inverse.append(r)
        left[k] = left[k] * r
        right[k] = right[k] * r
        for i in range(k + 1, SUB):
            a[i][k] = a[i][k] * r
        for i in range(k + 1, SUB):
            for j in range(k + 1, i + 1):
                a[i][j] = a[i][j] - a[i][k] * a[j][k]
            left[i] = left[i] - a[i][k] * left[k]
            right[i] = right[i] - a[i][k] * right[k]
    return a, inverse


def spread(rows):
    return [jnp.broadcast_to(rows[i : i + 1], rows.shape) for i in range(SUB)]


def gathered(rows):
    return jnp.concatenate([rows[i][i : i + 1] for i in range(SUB)], axis=0)


def factor_rows(ranks, state):
    step = 2 * SUB
    for lo in range(0, ranks, step):
        mid, hi = lo + SUB, lo + step
        left = spread(state[lo:mid, 0:ranks])
        right = spread(state[lo:mid, ranks : 2 * ranks])
        low_left = state[mid:hi, 0:ranks]
        low_right = state[mid:hi, ranks : 2 * ranks]
        start = [
            jnp.broadcast_to(low_left[:, lo + k : lo + k + 1], (SUB, ranks))
            for k in range(SUB)
        ]
        mult, inverse = eliminate(left, right, lo)
        cols = []
        for k in range(SUB):
            col = start[k]
            for j in range(k):
                col = col - cols[j] * mult[k][j]
            cols.append(col * inverse[k])
        for k in range(SUB):
            low_left = low_left - cols[k] * left[k]
            low_right = low_right - cols[k] * right[k]
        next_left, next_right = spread(low_left), spread(low_right)
        eliminate(next_left, next_right, mid)
        new_left = jnp.concatenate([gathered(left), gathered(next_left)], axis=0)
        new_right = jnp.concatenate([gathered(right), gathered(next_right)], axis=0)
        state[lo:hi, ranks : 2 * ranks] = new_right
        if hi < ranks:
            new = jnp.concatenate([new_left, new_right], axis=1)
            h, m, l = split3(new)
            lh, lm, ll = (x[:, 0:ranks] for x in (h, m, l))
            one = jnp.concatenate([lh, lh, lh, lm, lm, ll], axis=0).T[hi:ranks].astype(BF16)
            two = jnp.concatenate([h, m, l, h, m, h], axis=0).astype(BF16)
            state[hi:ranks, :] = state[hi:ranks, :] - jnp.dot(
                one, two, preferred_element_type=F32
            )


def pivot_side(dim, coords, centre):
    y = coords[0:dim, :] - centre
    yh, ym, yl = split3(y)
    nh, nm, nl = split3(-0.5 * jnp.sum(y * y, axis=0, keepdims=True))
    ones = jnp.ones_like(nh)
    tail = [ones, ones, ones, nh, nm, nl, jnp.zeros((dim - 6, y.shape[1]), F32)]
    return jnp.concatenate([yh, yh, ym, ym, yh, yl] + tail, axis=0).T.astype(BF16)


def point_side(dim, x):
    xh, xm, xl = split3(x)
    nh, nm, nl = split3(-0.5 * jnp.sum(x * x, axis=0, keepdims=True))
    ones = jnp.ones_like(nh)
    tail = [nh, nm, nl, ones, ones, ones, jnp.zeros((dim - 6, x.shape[1]), F32)]
    return jnp.concatenate([xh, xm, xh, xm, xl, xh] + tail, axis=0).astype(BF16)


def body_kernel(
    n, blocks, chunk,
    points, scales, noise, pivots,
    factor, residual, averages,
    packed, slots, state, after, sum_slots,
    send_sem, recv_sem, sum_send_sem, sum_recv_sem,
):
    dim, width = points.shape
    ranks = factor.shape[0]
    per_block = ranks // blocks
    me = lax.axis_index("rows")
    offset = me * width

    barrier = pltpu.get_barrier_semaphore()

    def greet(k, carry):
        pl.semaphore_signal(
            barrier, inc=1, device_id=(lax.rem(me + k, n),),
            device_id_type=pl.DeviceIdType.MESH,
        )
        return carry

    lax.fori_loop(1, n, greet, 0)
    load_points(dim, points, scales, noise, packed)
    pivot_row = jnp.concatenate([pivots[b : b + 1, :] for b in range(blocks)], axis=1)
    own = gather_own(ranks, offset, chunk, pivot_row, packed)
    for d in range(dim + 1):
        slots[0, d] = own[d : d + 1]
    pl.semaphore_wait(barrier, n - 1)
    exchange_start(n, me, slots, send_sem, recv_sem)
    coords = exchange_finish(n, me, slots, send_sem, recv_sem)
    coords = jnp.concatenate([coords[d] for d in range(dim + 1)], axis=0)

    cov, eye = pivot_covariance(dim, coords)
    state[:, 0:ranks] = cov
    state[:, ranks : 2 * ranks] = eye
    factor_rows(ranks, state)
    row = lax.broadcasted_iota(jnp.int32, (ranks, ranks), 0)
    col = lax.broadcasted_iota(jnp.int32, (ranks, ranks), 1)
    solve = jnp.where(row >= col, state[:, ranks : 2 * ranks], 0.0)

    centre = jnp.sum(coords[0:dim, :], axis=1, keepdims=True) / ranks
    side = pivot_side(dim, coords, centre)
    local_row = (pivot_row - offset).astype(F32)
    local_col = jnp.broadcast_to(local_row, (SUB, ranks)).T[:, 0:1].astype(jnp.int32)
    for c in range(width // chunk):
        at = slice(c * chunk, (c + 1) * chunk)
        x = packed[0:dim, at] - centre
        cross = jnp.exp(jnp.dot(side, point_side(dim, x), preferred_element_type=F32))
        noise_row = packed[dim : dim + 1, at]
        ids = lax.broadcasted_iota(jnp.int32, (ranks, chunk), 1) + c * chunk
        cross = cross + jnp.where(ids == local_col, noise_row, 0.0)
        rows = jnp.dot(
            solve, cross, precision=lax.Precision.HIGHEST, preferred_element_type=F32
        )
        factor[:, at] = rows
        left = 1.0 + noise_row
        for b in range(blocks):
            part = rows[b * per_block : (b + 1) * per_block]
            left = left - jnp.sum(part * part, axis=0, keepdims=True)
            after[b : b + 1, at] = left
        residual[at] = left[0]

    total = jnp.zeros((blocks, LANES), F32)
    for c in range(width // LANES):
        total = total + after[:, c * LANES : (c + 1) * LANES]
    total = jnp.sum(total, axis=1, keepdims=True)
    row = lax.broadcasted_iota(jnp.int32, (blocks, LANES), 0)
    col = lax.broadcasted_iota(jnp.int32, (blocks, LANES), 1)
    sum_slots[0] = jnp.sum(jnp.where(row == col, total, 0.0), axis=0, keepdims=True)
    exchange_start(n, me, sum_slots, sum_send_sem, sum_recv_sem)
    total = exchange_finish(n, me, sum_slots, sum_send_sem, sum_recv_sem)
    averages[...] = total[0, 0:blocks] / (width * n)


def store_kernel(factor, residual, averages, to_factor, to_residual, to_averages, sem):
    copies = [
        pltpu.make_async_copy(source, target, sem.at[i])
        for i, (source, target) in enumerate(
            [(factor, to_factor), (residual, to_residual), (averages, to_averages)]
        )
    ]
    for copy in copies:
        copy.start()
    for copy in copies:
        copy.wait()


def body(n, points, scales, noise_var, pivots):
    dim, width = points.shape
    blocks, per_block = pivots.shape
    ranks = blocks * per_block
    chunk = 512
    vmem = pl.BlockSpec(memory_space=pltpu.VMEM)
    factor, residual, averages = pl.pallas_call(
        functools.partial(body_kernel, n, blocks, chunk),
        name="whole",
        out_shape=(
            pltpu.VMEM((ranks, width), F32),
            pltpu.VMEM((width,), F32),
            pltpu.VMEM((blocks,), F32),
        ),
        in_specs=[
            vmem, pl.BlockSpec(memory_space=pltpu.SMEM), vmem, vmem,
        ],
        out_specs=(vmem, vmem, vmem),
        scratch_shapes=[
            pltpu.VMEM((2 * dim, width), F32),
            pltpu.VMEM((n, dim + 1, 1, ranks), F32),
            pltpu.VMEM((ranks, 2 * ranks), F32),
            pltpu.VMEM((blocks, width), F32),
            pltpu.VMEM((n, 1, LANES), F32),
            pltpu.SemaphoreType.DMA((n,)),
            pltpu.SemaphoreType.DMA((n,)),
            pltpu.SemaphoreType.DMA((n,)),
            pltpu.SemaphoreType.DMA((n,)),
        ],
        compiler_params=pltpu.CompilerParams(collective_id=0, has_side_effects=True),
    )(points, scales, noise_var.reshape(1, -1), pivots)
    anywhere = pl.BlockSpec(memory_space=pl.ANY)
    return pl.pallas_call(
        store_kernel,
        name="store",
        out_shape=(
            jax.ShapeDtypeStruct((ranks, width), F32),
            jax.ShapeDtypeStruct((width,), F32),
            jax.ShapeDtypeStruct((blocks,), F32),
        ),
        in_specs=[vmem] * 3,
        out_specs=(anywhere,) * 3,
        scratch_shapes=[pltpu.SemaphoreType.DMA((3,))],
    )(*(pltpu.with_memory_space_constraint(x, pltpu.VMEM) for x in (factor, residual, averages)))


def solution(mesh):
    in_specs = (P(None, "rows"), P(), P("rows"), P())
    out_specs = (P(None, "rows"), P("rows"), P())
    return jax.shard_map(
        functools.partial(body, mesh.shape["rows"]),
        mesh=mesh, in_specs=in_specs, out_specs=out_specs, check_vma=False,
    )
```
